32 devices in a mesh: section: 4 (over z), tx: 4 (over y, core), ty: 2 (over x).
Axes of the slice: x: 2, y: 2, z: 4, core: 2. Of those that a mesh axis runs over, the one named last changes fastest.
Arguments:
- state: bfloat16 [4, 2, 1, 4, 2, 8, 16, 768], P('section', None, None, 'tx', 'ty'), may hold values from -6 to 6
- w_qkv: bfloat16 [4, 768, 2304], P('section', ('tx', 'ty')), may hold values from -0.21875 to 0.21875
- w_out: bfloat16 [4, 768, 768], P('section', ('tx', 'ty')), may hold values from -0.21875 to 0.21875
- w_up: bfloat16 [4, 768, 3072], P('section', ('tx', 'ty')), may hold values from -0.21875 to 0.21875
- w_down: bfloat16 [4, 3072, 768], P('section', ('tx', 'ty')), may hold values from -0.109375 to 0.109375
Outputs:
- final_state: bfloat16 [4, 2, 1, 4, 2, 8, 16, 768], P('section', None, None, 'tx', 'ty')
The draws below stay inside these ranges and needn't reach their ends.
All inputs are finite; a program needn't handle non-finite values.
Results may differ from the reference program's by a relative error of at most 0.0085.
Values may be sent and summed in bfloat16 or wider, within the bound.
No kernel may reach another device: no remote copies, remote signals or barrier semaphores. Data moves between devices by JAX's collectives and lax.ppermute only.
A program may use at most 128 MiB of HBM per device.

```python
import jax
import jax.numpy as jnp
from jax import lax

D = 768
HEADS = 6
HEAD = 128
FF = 3072
WIN_H = 8
WIN_W = 16
WC = 1
SAMPLES = 2
TICKS = 2
INNER = 768
SECTIONS = 4
N_TX = 4
N_TY = 2


def block_scale(own_key, dims, split, smallest, high):
    def one(dim, shards_of):
        steps = jax.random.uniform(jax.random.fold_in(jax.random.fold_in(own_key, 6), dim), (shards_of,), jnp.float32, smallest / len(split), high / len(split))
        return jnp.repeat(jnp.exp(steps), dims[dim] // shards_of).reshape((-1,) + (1,) * (len(dims) - dim - 1))

    factor_of = one(*split[0])
    for cut in split[1:]:
        factor_of = factor_of * one(*cut)
    return factor_of


def scatter_about(rng, extent, spread, most, cuts=(), held_as=jnp.bfloat16):
    values = spread * jax.random.normal(rng, extent, jnp.float32)
    if cuts:
        values = values * block_scale(rng, extent, cuts, -0.22, 0.18)
    return jnp.clip(values, -most, most).astype(held_as)


def setup_inputs(seed: int = 0) -> dict:
    key_list = jax.random.split(jax.random.key(seed), 6)
    state = scatter_about(key_list[0], (SECTIONS, SAMPLES, WC, N_TX, N_TY, WIN_H, WIN_W, D), 1.0, 6.0, ((0, 4), (3, 4), (4, 2)))
    w_qkv = scatter_about(key_list[1], (SECTIONS, D, 3 * INNER), D ** -0.5, 0.21875, ((0, 4), (1, 8)))
    w_out = scatter_about(key_list[2], (SECTIONS, INNER, D), INNER ** -0.5, 0.21875, ((0, 4), (1, 8)))
    w_up = scatter_about(key_list[3], (SECTIONS, D, FF), D ** -0.5, 0.21875, ((0, 4), (1, 8)))
    w_down = scatter_about(key_list[4], (SECTIONS, FF, D), FF ** -0.5, 0.109375, ((0, 4), (1, 8)))
    return {"state": state, "w_qkv": w_qkv, "w_out": w_out, "w_up": w_up, "w_down": w_down}


epsilon = 1e-06

def rms_round(values):
    scale = lax.rsqrt(lax.optimization_barrier(jnp.mean(values * values, axis=-1, keepdims=True)) + epsilon)
    return (values * scale).astype(jnp.bfloat16)

def run_block(block, w_qkv, w_out, w_up, w_down, rolls_done):
    height = N_TX * WIN_H
    width = WC * N_TY * WIN_W
    window_len = WIN_H * WIN_W
    inner_width = HEADS * HEAD
    window_count = N_TX * WC * N_TY
    token_grid = block.transpose(1, 3, 0, 2, 4, 5).reshape(height, width, D)
    rolled = jnp.roll(token_grid, (-(WIN_H // 2), -(WIN_W // 2)), axis=(0, 1))
    windows = rolled.reshape(N_TX, WIN_H, WC * N_TY, WIN_W, D).transpose(0, 2, 1, 3, 4)
    tokens_float = windows.reshape(-1, D).astype(jnp.float32)
    normed = rms_round(tokens_float)
    qkv = jnp.dot(normed, w_qkv, preferred_element_type=jnp.float32)
    queries = (qkv[:, :inner_width] * HEAD ** (-0.5)).astype(jnp.bfloat16)
    queries = queries.reshape(window_count, window_len, HEADS, HEAD)
    key_heads = qkv[:, inner_width:2 * inner_width].astype(jnp.bfloat16)
    key_heads = key_heads.reshape(window_count, window_len, HEADS, HEAD)
    value_heads = qkv[:, 2 * inner_width:].astype(jnp.bfloat16)
    value_heads = value_heads.reshape(window_count, window_len, HEADS, HEAD)
    scores = jnp.einsum('wqhe,wkhe->whqk', queries.astype(jnp.float32), key_heads.astype(jnp.float32))
    row_index = jnp.arange(height, dtype=jnp.int32) + WIN_H // 2 * rolls_done
    row_band = (row_index // height).reshape(N_TX, WIN_H, 1)
    row_band = jnp.broadcast_to(row_band, (N_TX, WIN_H, WIN_W)).reshape(N_TX, 1, window_len)
    same_band = (row_band[:, :, :, None] == row_band[:, :, None, :]).astype(jnp.float32)
    exp_scores = jnp.exp(scores).reshape(N_TX, WC * N_TY, HEADS, window_len, window_len)
    exp_scores = exp_scores * same_band[:, :, None]
    softmax_out = (exp_scores / lax.optimization_barrier(jnp.sum(exp_scores, axis=-1, keepdims=True))).astype(jnp.bfloat16)
    softmax_out = softmax_out.reshape(window_count, HEADS, window_len, window_len)
    mixed_heads = jnp.einsum('whqk,wkhe->wqhe', softmax_out.astype(jnp.float32), value_heads.astype(jnp.float32))
    mixed_heads = mixed_heads.astype(jnp.bfloat16).reshape(-1, inner_width)
    residual = tokens_float + jnp.dot(mixed_heads, w_out, preferred_element_type=jnp.float32)
    hidden = jax.nn.gelu(jnp.dot(rms_round(residual), w_up, preferred_element_type=jnp.float32), approximate=True)
    hidden = hidden.astype(jnp.bfloat16)
    result = (residual + jnp.dot(hidden, w_down, preferred_element_type=jnp.float32)).astype(jnp.bfloat16)
    result = result.reshape(N_TX, WC * N_TY, WIN_H, WIN_W, D).transpose(0, 2, 1, 3, 4)
    return result.reshape(N_TX, WIN_H, WC, N_TY, WIN_W, D).transpose(2, 0, 3, 1, 4, 5)

def reference(state, w_qkv, w_out, w_up, w_down):
    current = state
    for step_index in range(TICKS):
        rolls_done = step_index + 1

        def section_step(operands):
            blocks, first_matrix, second_matrix, third_matrix, fourth_matrix = operands
            return jnp.stack([run_block(blocks[sample], first_matrix, second_matrix, third_matrix, fourth_matrix, rolls_done) for sample in range(SAMPLES)])
        outgoing = lax.map(section_step, (current, w_qkv, w_out, w_up, w_down))
        current = jnp.roll(outgoing, 1, axis=0)
    return current
```

```python
import functools

import jax
import jax.numpy as jnp
from jax import lax
from jax.experimental import pallas as pl
from jax.experimental.pallas import tpu as pltpu
from jax.sharding import PartitionSpec as P

HEAD = 128
TICKS = 2
epsilon = 1e-06


VMEM = pl.BlockSpec(memory_space=pltpu.VMEM)
SMEM = pl.BlockSpec(memory_space=pltpu.SMEM)
MIB = 1 << 20


def shift(x, section=0, tx=0, ty=0):
    n_s, n_x, n_y = (lax.axis_size(a) for a in ("section", "tx", "ty"))
    place = lambda s, i, j: ((s % n_s) * n_x + i % n_x) * n_y + j % n_y
    pairs = [
        (place(s, i, j), place(s + section, i + tx, j + ty))
        for s in range(n_s)
        for i in range(n_x)
        for j in range(n_y)
    ]
    return lax.ppermute(x, ("section", "tx", "ty"), pairs)


def swap(x, outer=0, inner=0, ty=0):
    n_x, n_y = lax.axis_size("tx"), lax.axis_size("ty")
    n_o = n_x // 2
    place = lambda o, i, j: ((o % n_o) * 2 + i % 2) * n_y + j % n_y
    pairs = [
        (place(o, i, j), place(o + outer, i + inner, j + ty))
        for o in range(n_o)
        for i in range(2)
        for j in range(n_y)
    ]
    return lax.ppermute(x, ("tx", "ty"), pairs)


def gather_rows(shard):
    n_x, n_y = lax.axis_size("tx"), lax.axis_size("ty")
    rows = shard.shape[0]
    if n_x != 4 or n_y != 2 or rows % 16:
        return [lax.all_gather(shard, ("tx", "ty"), axis=0, tiled=True)], [jnp.int32(0)]
    half = rows // 2
    i, j = lax.axis_index("tx"), lax.axis_index("ty")
    across_y = swap(shard, ty=1)
    across_o = swap(shard, outer=1)
    first = swap(across_y[:half], outer=1)
    second = swap(across_o[half:], ty=1)
    pieces = [shard, across_y, across_o, first, second]

    def begins(i):
        at = lambda i, j: (i * n_y + j) * rows
        far = at((i + 2) % 4, 1 - j)
        return [at(i, j), at(i, 1 - j), at((i + 2) % 4, j), far, far + half]

    mate = i + 1 - 2 * (i % 2)
    return pieces + [swap(p, inner=1) for p in pieces], begins(i) + begins(mate)


def rms_round(values):
    scale = lax.rsqrt(jnp.mean(values * values, axis=-1, keepdims=True) + epsilon)
    return (values * scale).astype(jnp.bfloat16)


def dot(a, b):
    return jnp.dot(a, b, preferred_element_type=jnp.float32)


def assemble(begins, pieces, whole):
    for n, piece in enumerate(pieces):
        rows = piece.shape[0]
        whole[pl.ds(pl.multiple_of(begins[n], 8), rows), :] = piece[...]


def attention(split, tokens, w_qkv, w_out, qkv, mixed, window_len, cols):
    inner = w_out.shape[0]
    normed = rms_round(tokens)
    for part in range(3):
        there = slice(part * inner, (part + 1) * inner)
        out = dot(normed, w_qkv[:, there])
        if part == 0:
            out = out * HEAD ** (-0.5)
        qkv[:, there] = out.astype(jnp.bfloat16)
    row = lax.broadcasted_iota(jnp.int32, (window_len, window_len), 0) // cols >= split
    col = lax.broadcasted_iota(jnp.int32, (window_len, window_len), 1) // cols >= split
    same_band = row == col
    for w in range(tokens.shape[0] // window_len):
        rows = slice(w * window_len, (w + 1) * window_len)
        for h in range(inner // HEAD):
            take = lambda part: qkv[rows, part * inner + h * HEAD : part * inner + (h + 1) * HEAD]
            scores = lax.dot_general(
                take(0), take(1), (((1,), (1,)), ((), ())), preferred_element_type=jnp.float32
            )
            weights = jnp.where(same_band, jnp.exp(scores), 0.0)
            probs = (weights / jnp.sum(weights, axis=-1, keepdims=True)).astype(jnp.bfloat16)
            mixed[rows, h * HEAD : (h + 1) * HEAD] = dot(probs, take(2)).astype(jnp.bfloat16)
    return tokens + dot(mixed[...], w_out[...])


def gelu(values):
    return jax.nn.gelu(values, approximate=True)


def up(normed, w_up, hidden, tile):
    for n in range(w_up.shape[1] // tile):
        there = slice(n * tile, (n + 1) * tile)
        hidden[:, there] = gelu(dot(normed, w_up[:, there])).astype(jnp.bfloat16)


def read_tokens(quarters, tokens):
    hr, hc = quarters[0].shape[1:3]
    for n, quarter in enumerate(quarters):
        a, b = divmod(n, 2)
        tokens[:, a * hr : (a + 1) * hr, b * hc : (b + 1) * hc, :] = quarter[...].astype(jnp.float32)
    return tokens[...].reshape(-1, tokens.shape[-1])


def write_quarters(result, quarters):
    hr, hc, width = quarters[0].shape[1:]
    result = result.reshape(-1, 2 * hr, 2 * hc, width)
    for n, quarter in enumerate(quarters):
        a, b = divmod(n, 2)
        quarter[...] = result[:, a * hr : (a + 1) * hr, b * hc : (b + 1) * hc, :].astype(jnp.bfloat16)


def call(kernel, out_shape, scratch, operands, name, flops, limit=28):
    specs = [SMEM if o.dtype == jnp.int32 else VMEM for o in operands]
    return pl.pallas_call(
        kernel,
        out_shape=out_shape,
        in_specs=specs,
        out_specs=jax.tree.map(lambda _: VMEM, out_shape),
        scratch_shapes=scratch,
        compiler_params=pltpu.CompilerParams(vmem_limit_bytes=limit * MIB),
        cost_estimate=pl.CostEstimate(flops=flops, bytes_accessed=MIB, transcendentals=0),
        name=name,
    )(*operands)


def first_attention(split, quarters, qkv_pieces, out_pieces):
    (qkv_parts, qkv_begin), (out_parts, out_begin) = qkv_pieces, out_pieces
    windows, hr, hc, width = quarters[0].shape
    count = windows * hr * hc * 4
    qkv_width, inner = qkv_parts[0].shape[1], out_parts[0].shape[1]
    inner = qkv_width // 3
    n_q, n_o = len(qkv_parts), len(out_parts)

    def kernel(*refs):
        split, qb, ob = refs[:3]
        quarters, refs = refs[3:7], refs[7:]
        qp, op, refs = refs[:n_q], refs[n_q : n_q + n_o], refs[n_q + n_o :]
        residual, normed, w_qkv, w_out, tokens, qkv, mixed = refs
        assemble(qb, qp, w_qkv)
        assemble(ob, op, w_out)
        values = read_tokens(quarters, tokens)
        out = attention(split[0], values, w_qkv, w_out, qkv, mixed, 4 * hr * hc, 2 * hc)
        residual[...] = out
        normed[...] = rms_round(out)

    return call(
        kernel,
        (
            jax.ShapeDtypeStruct((count, width), jnp.float32),
            jax.ShapeDtypeStruct((count, width), jnp.bfloat16),
            jax.ShapeDtypeStruct((width, qkv_width), jnp.bfloat16),
            jax.ShapeDtypeStruct((inner, width), jnp.bfloat16),
        ),
        [
            pltpu.VMEM((windows, 2 * hr, 2 * hc, width), jnp.float32),
            pltpu.VMEM((count, qkv_width), jnp.bfloat16),
            pltpu.VMEM((count, inner), jnp.bfloat16),
        ],
        [split, jnp.stack(qkv_begin), jnp.stack(out_begin), *quarters, *qkv_parts, *out_parts],
        "first_attention",
        2 * count * width * (qkv_width + inner),
    )


def first_up(normed, pieces):
    parts, begin = pieces
    count, width = normed.shape
    wide = parts[0].shape[1]

    def kernel(begin, normed, *refs):
        hidden, w_up = refs[-2:]
        assemble(begin, refs[:-2], w_up)
        up(normed[...], w_up, hidden, width)

    return call(
        kernel,
        (
            jax.ShapeDtypeStruct((count, wide), jnp.bfloat16),
            jax.ShapeDtypeStruct((width, wide), jnp.bfloat16),
        ),
        [],
        [jnp.stack(begin), normed, *parts],
        "first_up",
        2 * count * width * wide,
    )


def first_down(residual, hidden, pieces, quarter_shape):
    parts, begin = pieces
    count, width = residual.shape
    wide = hidden.shape[1]

    def kernel(begin, residual, hidden, *refs):
        quarters, w_down = refs[-5:-1], refs[-1]
        assemble(begin, refs[:-5], w_down)
        write_quarters(residual[...] + dot(hidden[...], w_down[...]), quarters)

    return call(
        kernel,
        (
            *(jax.ShapeDtypeStruct(quarter_shape, jnp.bfloat16),) * 4,
            jax.ShapeDtypeStruct((wide, width), jnp.bfloat16),
        ),
        [],
        [jnp.stack(begin), residual, hidden, *parts],
        "first_down",
        2 * count * width * wide,
    )


def whole_block(split, quarters, matrices, last):
    w_qkv, w_out, w_up, w_down = matrices
    windows, hr, hc, width = quarters[0].shape
    count = windows * hr * hc * 4
    wide = w_up.shape[1]

    def kernel(split, q0, q1, q2, q3, w_qkv, w_out, w_up, w_down, *refs):
        *outs, tokens, qkv, mixed, hidden = refs
        values = read_tokens((q0, q1, q2, q3), tokens)
        residual = attention(split[0], values, w_qkv, w_out, qkv, mixed, 4 * hr * hc, 2 * hc)
        up(rms_round(residual), w_up, hidden, width)
        result = residual + dot(hidden[...], w_down[...])
        if last:
            outs[0][...] = result.astype(jnp.bfloat16)
        else:
            write_quarters(result, outs)

    if last:
        out_shape = (jax.ShapeDtypeStruct((count, width), jnp.bfloat16),)
    else:
        out_shape = (jax.ShapeDtypeStruct((windows, hr, hc, width), jnp.bfloat16),) * 4
    return call(
        kernel,
        out_shape,
        [
            pltpu.VMEM((windows, 2 * hr, 2 * hc, width), jnp.float32),
            pltpu.VMEM((count, w_qkv.shape[1]), jnp.bfloat16),
            pltpu.VMEM((count, w_out.shape[0]), jnp.bfloat16),
            pltpu.VMEM((count, wide), jnp.bfloat16),
        ],
        [split, *quarters, *matrices],
        "whole_block",
        2 * count * width * (w_qkv.shape[1] + w_out.shape[0] + 2 * wide),
    )


def roll_quarters(quarters, blocks, relay):
    upper_left, upper_right, lower_left, lower_right = quarters
    last = lax.axis_index("ty") == lax.axis_size("ty") - 1

    def from_right(x, tx):
        x = shift(x, section=relay, tx=tx, ty=-1)
        if blocks == 1:
            return x
        by_block = x.reshape(-1, blocks, *x.shape[1:])
        return jnp.where(last, jnp.roll(by_block, -1, axis=1), by_block).reshape(x.shape)

    here = shift(lower_right, section=relay) if relay else lower_right
    return (
        here,
        from_right(lower_left, 0),
        shift(upper_right, section=relay, tx=-1),
        from_right(upper_left, -1),
    )


def local(state, w_qkv, w_out, w_up, w_down):
    blocks = state.shape[2]
    win_rows, win_cols, width = state.shape[5:]
    hr, hc = win_rows // 2, win_cols // 2
    height = lax.axis_size("tx") * win_rows
    pieces = [gather_rows(w[0]) for w in (w_qkv, w_out, w_up, w_down)]
    windows = state.reshape(-1, win_rows, win_cols, width)
    quarters = [
        windows[:, a * hr : (a + 1) * hr, b * hc : (b + 1) * hc] for a in range(2) for b in range(2)
    ]
    quarters = roll_quarters(quarters, blocks, 0)
    matrices = None
    for tick in range(TICKS):
        split = (-(lax.axis_index("tx") * win_rows + hr * (tick + 1))) % height
        split = split.astype(jnp.int32).reshape(1)
        last = tick == TICKS - 1
        if tick == 0 and not last:
            residual, normed, whole_qkv, whole_out = first_attention(split, quarters, pieces[0], pieces[1])
            hidden, whole_up = first_up(normed, pieces[2])
            *quarters, whole_down = first_down(residual, hidden, pieces[3], quarters[0].shape)
            matrices = (whole_qkv, whole_out, whole_up, whole_down)
        else:
            outs = whole_block(split, quarters, matrices, last)
            if last:
                return shift(outs[0], section=1).reshape(state.shape)
            quarters = outs
        quarters = roll_quarters(quarters, blocks, 1)


def solution(mesh):
    weights = P("section", ("tx", "ty"), None)
    tokens = P("section", None, None, "tx", "ty", None, None, None)
    return jax.shard_map(
        local,
        mesh=mesh,
        in_specs=(tokens, weights, weights, weights, weights),
        out_specs=tokens,
        check_vma=False,
    )
```
